128 devices in a mesh: wide: 64 (over x, z, y), narrow: 2 (over core).
Axes of the slice: x: 4, y: 4, z: 4, core: 2. Of those that a mesh axis runs over, the one named last changes fastest.
Arguments:
- contributions: float32 [2, 3, 32768, 128], P('narrow', None, 'wide'), may hold values from -6 to 6
- send_map: int32 [64, 896], P('wide'), may hold values from -1 to 511, as said below
- arrival_map: int32 [64, 896], P('wide'), may hold values from -1 to 255, as said below
- dual_diagonal: float32 [16384, 128], P('wide'), may hold values from 0.5 to 2
- mortar: bfloat16 [16384, 128, 128], P('wide'), may hold values from -0.5 to 0.5
- master_inverse: bfloat16 [16384, 128, 128], P('wide'), may hold values from -0.5 to 0.5
Outputs:
- corrections: float32 [2, 3, 32768, 128], P('narrow', None, 'wide')
The draws below stay inside these ranges and needn't reach their ends.
Inputs may be any that keep to these rules, and one draw needn't show every extreme that they name: `send_map`: each row 0 to 511 of a partition stands in exactly one of its slots. Some stripe has all 14 of its slots used by every partition. arrival_map[d, o * 14 + c] is -1 exactly where send_map[o, d * 14 + c] is -1.
All inputs are finite; a program needn't handle non-finite values.
Results may differ from the reference program's by a relative error of at most 0.0041.
Values sent between devices are 32-bit elements; how exact they have to be, the bound alone decides.
A program may use at most 64 MiB of HBM per device.

```python
import math
import jax
import jax.numpy as jnp
from jax import lax

NODES = 128
COMP = 3
BLK_DEV = 256
BLOCKS = 16384
ROWS_OWN = 512
ROWS = 32768
CAP = 14
SLOTS = 896
N_WIDE = 64


def shared_maps(key):
    base = jax.random.fold_in(key, 7)
    key_hot, key_bias, key_jitter, key_tie, key_rows, key_block = jax.random.split(base, 6)
    hot_stripe = jax.random.randint(key_hot, (), 0, N_WIDE)
    stripe_bias = jax.random.randint(key_bias, (N_WIDE,), 0, 4)
    stripe_bias = stripe_bias * stripe_bias
    stripe_ids = jnp.arange(SLOTS, dtype=jnp.int32) // CAP
    random_perturbation = jax.random.randint(key_jitter, (N_WIDE, SLOTS), 0, 16)
    scores = jnp.where(stripe_ids[None, :] == hot_stripe, 1000, stripe_bias[stripe_ids][None, :] + random_perturbation)
    raw_ties = jax.random.randint(key_tie, (N_WIDE, SLOTS), 0, 1 << 30)
    tie_rank = jnp.argsort(jnp.argsort(raw_ties, axis=1), axis=1)
    priority_order = jnp.argsort(-(scores * SLOTS + tie_rank), axis=1)
    chosen = priority_order[:, :ROWS_OWN]
    row_order = jnp.argsort(jax.random.randint(key_rows, (N_WIDE, ROWS_OWN), 0, 1 << 30), axis=1).astype(jnp.int32)
    owners = jnp.arange(N_WIDE, dtype=jnp.int32)[:, None]
    send_map = jnp.full((N_WIDE, SLOTS), -1, jnp.int32).at[owners, chosen].set(row_order)
    by_stripe = jnp.transpose(send_map.reshape(N_WIDE, N_WIDE, CAP), (1, 0, 2)).reshape(N_WIDE, SLOTS)
    local_ids = jax.random.randint(key_block, (N_WIDE, SLOTS), 0, BLK_DEV)
    arrival_map = jnp.where(by_stripe >= 0, local_ids, -1).astype(jnp.int32)
    return (send_map, arrival_map)


def draw_send_map(key, part):
    return shared_maps(key)[0]


def draw_arrival_map(key, part):
    return shared_maps(key)[1]


def steps_of(key, shape, cuts, least, largest):
    def one(axis_at, shards_of):
        steps = jax.random.uniform(jax.random.fold_in(jax.random.fold_in(key, 6), axis_at), (shards_of,), jnp.float32, least / len(cuts), largest / len(cuts))
        return jnp.repeat(jnp.exp(steps), shape[axis_at] // shards_of).reshape((-1,) + (1,) * (len(shape) - axis_at - 1))

    level = one(*cuts[0])
    for cut in cuts[1:]:
        level = level * one(*cut)
    return level


def bell_draw(rng, shape, scale, most, cuts=(), kind=jnp.bfloat16):
    drawn = scale * jax.random.normal(rng, shape, jnp.float32)
    if cuts:
        drawn = drawn * steps_of(rng, shape, cuts, -0.22, 0.18)
    return jnp.clip(drawn, -most, most).astype(kind)


def setup_inputs(seed: int = 0) -> dict:
    seeds = jax.random.split(jax.random.key(seed), 7)
    return {
        "contributions": bell_draw(seeds[0], (2, COMP, ROWS, NODES), 1.0, 6.0, ((0, 2), (2, 64)), jnp.float32),
        "send_map": draw_send_map(jax.random.fold_in(seeds[6], 71), 0),
        "arrival_map": draw_arrival_map(jax.random.fold_in(seeds[6], 71), 0),
        "dual_diagonal": jnp.clip(jnp.exp(math.log(2.0) - 1.3862944 * jax.random.uniform(seeds[3], (BLOCKS, NODES), jnp.float32) ** steps_of(seeds[3], (BLOCKS, NODES), ((0, 64),), -0.2, 0.2)), 0.5, 2.0),
        "mortar": bell_draw(seeds[4], (BLOCKS, NODES, NODES), NODES ** -0.5, 0.5, ((0, 64),)),
        "master_inverse": bell_draw(seeds[5], (BLOCKS, NODES, NODES), NODES ** -0.5, 0.5, ((0, 64),)),
    }


def stripe_solve(pieces):
    summed, diagonal, mortar_part, inverse_part = pieces
    mortar_wide = mortar_part.astype(jnp.float32)
    inverse_wide = inverse_part.astype(jnp.float32)
    multiplier = summed[0] / diagonal[None]
    multiplier_low = lax.optimization_barrier(multiplier.astype(jnp.bfloat16)).astype(jnp.float32)
    pushed = jnp.einsum('bij,cbi->cbj', mortar_wide, multiplier_low, precision=lax.Precision.HIGHEST)
    condensed = summed[1] + pushed
    condensed_low = lax.optimization_barrier(condensed.astype(jnp.bfloat16)).astype(jnp.float32)
    master_fix = jnp.einsum('bkj,cbj->cbk', inverse_wide, condensed_low, precision=lax.Precision.HIGHEST)
    master_low = lax.optimization_barrier(master_fix.astype(jnp.bfloat16)).astype(jnp.float32)
    slave_fix = jnp.einsum('bij,cbj->cbi', mortar_wide, master_low, precision=lax.Precision.HIGHEST) / diagonal[None]
    return jnp.stack([slave_fix, master_fix])


def reference(contributions, send_map, arrival_map, dual_diagonal, mortar, master_inverse):
    owners = jnp.arange(N_WIDE, dtype=jnp.int32)[:, None]
    slot_ids = jnp.arange(SLOTS, dtype=jnp.int32)[None, :]
    stripes = slot_ids // CAP
    local_block = arrival_map[stripes, owners * CAP + slot_ids % CAP]
    is_live = send_map >= 0
    targets = jnp.where(is_live, owners * ROWS_OWN + send_map, ROWS).astype(jnp.int32)
    block_ids = (stripes * BLK_DEV + local_block).astype(jnp.int32)
    row_block = jnp.zeros((ROWS + 1,), jnp.int32).at[targets.reshape(-1)].set(block_ids.reshape(-1))[:ROWS]
    summed = jnp.zeros((2, COMP, BLOCKS, NODES), jnp.float32).at[:, :, row_block, :].add(contributions)
    by_stripe = jnp.transpose(summed.reshape(2, COMP, N_WIDE, BLK_DEV, NODES), (2, 0, 1, 3, 4))
    diag_parts = dual_diagonal.reshape(N_WIDE, BLK_DEV, NODES)
    mortar_parts = mortar.reshape(N_WIDE, BLK_DEV, NODES, NODES)
    inverse_parts = master_inverse.reshape(N_WIDE, BLK_DEV, NODES, NODES)
    fixes = lax.map(stripe_solve, (by_stripe, diag_parts, mortar_parts, inverse_parts))
    fixes = jnp.transpose(fixes, (1, 2, 0, 3, 4)).reshape(2, COMP, BLOCKS, NODES)
    return fixes[:, :, row_block, :]
```

```python
import functools
import jax
import jax.numpy as jnp
from jax import lax
from jax.experimental import pallas as pl
from jax.experimental.pallas import tpu as pltpu
from jax.sharding import PartitionSpec as P

MESH = pl.DeviceIdType.MESH
F32 = jnp.float32
BF16 = jnp.bfloat16
N_WIDE = 64
CAP = 14
PAD = 16
ROWS = 512
BLK = 256
HALF = 128
NODES = 128
SLOTS = N_WIDE * PAD
GROUPS = ((0,), (1,), (2,))


def dot(a, b):
    return lax.dot_general(a, b, (((1,), (0,)), ((), ())), preferred_element_type=F32)


def dot_nt(a, b):
    return lax.dot_general(a, b, (((1,), (1,)), ((), ())), preferred_element_type=F32)


def split(x):
    hi = x.astype(BF16)
    lo = (x - hi.astype(F32)).astype(BF16)
    return jnp.concatenate([hi, lo], axis=1)


def padded_map(ref):
    x = jnp.concatenate([ref[:, 112 * r : 112 * (r + 1)] for r in range(8)], axis=0) + 1
    hi = (x >> 4).astype(F32).astype(BF16)
    lo = (x & 15).astype(F32).astype(BF16)
    i = lax.broadcasted_iota(jnp.int32, (112, 128), 0)
    l = lax.broadcasted_iota(jnp.int32, (112, 128), 1)
    q = jnp.where((i == (l >> 4) * CAP + (l & 15)) & ((l & 15) < CAP), 1.0, 0.0).astype(BF16)
    rows = dot(hi, q) * 16.0 + dot(lo, q) - 1.0
    cols = jnp.transpose(jnp.concatenate([rows] * 16, axis=0))
    return rows.astype(jnp.int32), cols.astype(jnp.int32)


def one_hot_cols(cols, out_ref, width):
    lane = lax.broadcasted_iota(jnp.int32, (128, width), 1)
    for r in range(8):
        out_ref[pl.ds(128 * r, 128), :] = jnp.where(cols[:, r : r + 1] == lane, 1.0, 0.0).astype(BF16)


def one_hot_rows(rows, out_ref, height):
    sub = lax.broadcasted_iota(jnp.int32, (height, 128), 0)
    for r in range(8):
        out_ref[:, pl.ds(128 * r, 128)] = jnp.where(rows[r : r + 1, :] == sub, 1.0, 0.0).astype(BF16)


def kernel(
    contrib_ref, smap_ref, amap_ref, diag_ref, mortar_hbm, inv_hbm, out_ref,
    send, recv, back, home, s_col, s_row, a_col, a_row, mortar, inverse,
    sums, other, vec, mid, fix, fixed_in,
    load_sem, send_sem, recv_sem, xs_sem, xr_sem,
):
    w = lax.axis_index("wide")
    n = lax.axis_index("narrow")
    x0, z0, y0 = w // 16, (w // 4) % 4, w % 4

    def peer(k):
        k = 64 - k
        return ((x0 + k // 16) % 4) * 16 + ((z0 + (k // 4) % 4) % 4) * 4 + (y0 + k % 4) % 4

    barrier = pltpu.get_barrier_semaphore()

    @pl.loop(1, N_WIDE)
    def _(k):
        pl.semaphore_signal(barrier, inc=1, device_id={"wide": peer(k)}, device_id_type=MESH)

    pl.semaphore_signal(barrier, inc=1, device_id={"narrow": 1 - n}, device_id_type=MESH)

    first = pl.multiple_of(n * HALF, HALF)
    load_m = pltpu.make_async_copy(mortar_hbm.at[pl.ds(first, HALF)], mortar, load_sem.at[0])
    load_i = pltpu.make_async_copy(inv_hbm.at[pl.ds(first, HALF)], inverse, load_sem.at[1])
    load_m.start()
    load_i.start()

    def exchange(src, dst, leg, c):
        @pl.loop(1, N_WIDE)
        def _(k):
            p = peer(k)
            pltpu.make_async_remote_copy(
                src_ref=src.at[c, p, pl.ds(0, CAP)],
                dst_ref=dst.at[c, w, pl.ds(0, CAP)],
                send_sem=send_sem.at[leg, c],
                recv_sem=recv_sem.at[leg, c],
                device_id={"wide": p},
                device_id_type=MESH,
            ).start()

        dst[c, pl.ds(w, 1)] = src[c, pl.ds(w, 1)]

    def all_bytes(buf, sem, c):
        ref = buf.at[c, pl.ds(0, N_WIDE - 1), pl.ds(0, CAP)]
        return pltpu.make_async_copy(ref, ref, sem)

    def swap(src, dst, leg, c):
        return pltpu.make_async_remote_copy(
            src_ref=src, dst_ref=dst, send_sem=xs_sem.at[leg, c], recv_sem=xr_sem.at[leg, c],
            device_id={"narrow": 1 - n}, device_id_type=MESH,
        )

    s_rows, s_cols = padded_map(smap_ref)
    one_hot_cols(s_cols, s_col, ROWS)
    zero = jnp.zeros((N_WIDE, PAD - CAP, NODES), F32)
    for c in range(3):
        recv[c, :, pl.ds(CAP, PAD - CAP), :] = zero
        home[c, :, pl.ds(CAP, PAD - CAP), :] = zero

    for c in range(3):
        both = dot(s_col[...], split(contrib_ref[0, c]))
        send[c] = (both[:, :NODES] + both[:, NODES:]).reshape(N_WIDE, PAD, NODES)
        if c == 0:
            pl.semaphore_wait(barrier, N_WIDE)
        exchange(send, recv, 0, c)

    one_hot_rows(s_rows, s_row, ROWS)
    a_rows, a_cols = padded_map(amap_ref)
    one_hot_rows(a_rows, a_row, BLK)
    one_hot_cols(a_cols, a_col, BLK)
    mine = pl.ds(first, HALF)
    theirs = pl.ds(pl.multiple_of((1 - n) * HALF, HALF), HALF)
    diag = diag_ref[mine, :]
    load_m.wait()
    load_i.wait()

    sub = lax.broadcasted_iota(jnp.int32, (8, NODES), 0)

    for group in GROUPS:
        for c in group:
            all_bytes(recv, recv_sem.at[0, c], c).wait()
            both = dot(a_row[...], split(recv[c].reshape(SLOTS, NODES)))
            sums[c] = both[:, :NODES] + both[:, NODES:]
            swap(sums.at[c, theirs], other.at[c], 0, c).start()
        for c in group:
            swap(sums.at[c, theirs], other.at[c], 0, c).wait()
            own = sums[c, mine, :]
            got = other[c]
            slave = jnp.where(n == 0, own, got)
            master = jnp.where(n == 0, got, own)
            vec[c] = slave / diag
            mid[c] = master

        def stage(mats, src, transposed, finish):
            @pl.loop(0, HALF // 16)
            def _(g):
                for h in range(2):
                    at = pl.ds(pl.multiple_of(g * 16 + h * 8, 8), 8)
                    parts = [src[c, at, :] for c in group]
                    acc = [jnp.zeros((8, NODES), F32)] * len(group)
                    total = None
                    for b in range(8):
                        mat = mats[g * 16 + h * 8 + b]
                        left = jnp.concatenate(
                            [jnp.where(sub == b, v, 0.0) for v in parts], axis=0
                        ).astype(BF16)
                        got = dot_nt(left, mat) if transposed else dot(left, mat)
                        total = got if total is None else total + got
                    for i, c in enumerate(group):
                        finish(c, at, total[8 * i : 8 * i + 8])

        def after_push(c, at, v):
            mid[c, at, :] = mid[c, at, :] + v

        def after_master(c, at, v):
            fix[c, 1, at, :] = v
            vec[c, at, :] = v

        def after_slave(c, at, v):
            fix[c, 0, at, :] = v / diag_ref[pl.ds(first + at.start, 8), :]

        stage(mortar, vec, False, after_push)
        stage(inverse, mid, True, after_master)
        stage(mortar, vec, True, after_slave)

        for c in group:
            swap(fix.at[c, 1 - n], fixed_in.at[c], 1, c).start()
        for c in group:
            swap(fix.at[c, 1 - n], fixed_in.at[c], 1, c).wait()
            own = fix[c, pl.ds(n, 1)][0]
            got = fixed_in[c]
            low = jnp.where(n == 0, own, got)
            high = jnp.where(n == 0, got, own)
            full = jnp.concatenate([low, high], axis=0).astype(BF16)
            back[c] = dot(a_col[...], full).reshape(N_WIDE, PAD, NODES)
            exchange(back, home, 1, c)

    for c in range(3):
        all_bytes(home, recv_sem.at[1, c], c).wait()
        out_ref[0, c] = dot(s_row[...], home[c].reshape(SLOTS, NODES).astype(BF16))

    for c in range(3):
        all_bytes(send, send_sem.at[0, c], c).wait()
        all_bytes(back, send_sem.at[1, c], c).wait()


def shards(contributions, send_map, arrival_map, dual_diagonal, mortar, master_inverse):
    vmem = pl.BlockSpec(memory_space=pltpu.VMEM)
    hbm = pl.BlockSpec(memory_space=pl.ANY)
    packets = pltpu.VMEM((3, N_WIDE, PAD, NODES), F32)
    return pl.pallas_call(
        kernel,
        out_shape=jax.ShapeDtypeStruct(contributions.shape, F32),
        in_specs=[vmem, vmem, vmem, vmem, hbm, hbm],
        out_specs=vmem,
        scratch_shapes=[
            packets, packets, packets, packets,
            pltpu.VMEM((SLOTS, ROWS), BF16),
            pltpu.VMEM((ROWS, SLOTS), BF16),
            pltpu.VMEM((SLOTS, BLK), BF16),
            pltpu.VMEM((BLK, SLOTS), BF16),
            pltpu.VMEM((HALF, NODES, NODES), BF16),
            pltpu.VMEM((HALF, NODES, NODES), BF16),
            pltpu.VMEM((3, BLK, NODES), F32),
            pltpu.VMEM((3, HALF, NODES), F32),
            pltpu.VMEM((3, HALF, NODES), F32),
            pltpu.VMEM((3, HALF, NODES), F32),
            pltpu.VMEM((3, 2, HALF, NODES), F32),
            pltpu.VMEM((3, HALF, NODES), F32),
            pltpu.SemaphoreType.DMA((2,)),
            pltpu.SemaphoreType.DMA((2, 3)),
            pltpu.SemaphoreType.DMA((2, 3)),
            pltpu.SemaphoreType.DMA((2, 3)),
            pltpu.SemaphoreType.DMA((2, 3)),
        ],
        compiler_params=pltpu.CompilerParams(
            collective_id=0, has_side_effects=True, vmem_limit_bytes=56 * 1024 * 1024
        ),
        name="mortar",
    )(contributions, send_map, arrival_map, dual_diagonal, mortar, master_inverse)


def solution(mesh):
    placed = (
        P("narrow", None, "wide", None),
        P("wide", None),
        P("wide", None),
        P("wide", None),
        P("wide", None, None),
        P("wide", None, None),
    )
    return jax.shard_map(
        shards,
        mesh=mesh,
        in_specs=placed,
        out_specs=P("narrow", None, "wide", None),
        check_vma=False,
    )
```

```python
import functools
import jax
import jax.numpy as jnp
from jax import lax
from jax.experimental import pallas as pl
from jax.experimental.pallas import tpu as pltpu
from jax.sharding import PartitionSpec as P

MESH = pl.DeviceIdType.MESH
F32 = jnp.float32
BF16 = jnp.bfloat16
N_WIDE = 64
CAP = 14
PAD = 16
ROWS = 512
BLK = 256
HALF = 128
NODES = 128
SLOTS = N_WIDE * PAD
CHUNK = 128


def hops(o):
    return sum(min(v, 4 - v) for v in o)


OFFSETS = sorted(
    ((i // 16, (i // 4) % 4, i % 4) for i in range(1, N_WIDE)),
    key=lambda o: (-hops(o), (o[0] * 5 + o[1] * 3 + o[2] * 7) % 11),
)


def dot(a, b):
    return lax.dot_general(a, b, (((1,), (0,)), ((), ())), preferred_element_type=F32)


def dot_nt(a, b):
    return lax.dot_general(a, b, (((1,), (1,)), ((), ())), preferred_element_type=F32)


def split(x):
    hi = x.astype(BF16)
    lo = (x - hi.astype(F32)).astype(BF16)
    return jnp.concatenate([hi, lo], axis=1)


def padded_map(ref):
    x = jnp.concatenate([ref[:, 112 * r : 112 * (r + 1)] for r in range(8)], axis=0) + 1
    hi = (x >> 4).astype(F32).astype(BF16)
    lo = (x & 15).astype(F32).astype(BF16)
    i = lax.broadcasted_iota(jnp.int32, (112, 128), 0)
    l = lax.broadcasted_iota(jnp.int32, (112, 128), 1)
    q = jnp.where((i == (l >> 4) * CAP + (l & 15)) & ((l & 15) < CAP), 1.0, 0.0).astype(BF16)
    rows = dot(hi, q) * 16.0 + dot(lo, q) - 1.0
    cols = jnp.transpose(jnp.concatenate([rows] * 16, axis=0))
    return rows.astype(jnp.int32), cols.astype(jnp.int32)


def one_hot_cols(cols, out_ref, width):
    lane = lax.broadcasted_iota(jnp.int32, (128, width), 1)
    for r in range(8):
        out_ref[pl.ds(128 * r, 128), :] = jnp.where(cols[:, r : r + 1] == lane, 1.0, 0.0).astype(BF16)


def one_hot_rows(rows, out_ref, height):
    sub = lax.broadcasted_iota(jnp.int32, (height, 128), 0)
    for r in range(8):
        out_ref[:, pl.ds(128 * r, 128)] = jnp.where(rows[r : r + 1, :] == sub, 1.0, 0.0).astype(BF16)


def kernel(
    contrib_hbm, smap_hbm, amap_hbm, diag_hbm, mortar_hbm, inv_hbm, out_ref,
    contrib, smap, amap, diag, send, recv, back, home,
    s_col, s_row, a_col, a_row, mortar, mortar_t, inverse,
    sums, other, vec, mid, fix, fixed_in,
    load_sem, send_sem, recv_sem, xs_sem, xr_sem,
):
    w = lax.axis_index("wide")
    n = lax.axis_index("narrow")
    x0, z0, y0 = w // 16, (w // 4) % 4, w % 4
    xs = [(x0 + i) % 4 * 16 for i in range(4)]
    zs = [(z0 + i) % 4 * 4 for i in range(4)]
    ys = [(y0 + i) % 4 for i in range(4)]
    peers = [xs[i] + zs[j] + ys[k] for i, j, k in OFFSETS]

    barrier = pltpu.get_barrier_semaphore()
    for p in peers:
        pl.semaphore_signal(barrier, inc=1, device_id={"wide": p}, device_id_type=MESH)
    pl.semaphore_signal(barrier, inc=1, device_id={"narrow": 1 - n}, device_id_type=MESH)

    first = pl.multiple_of(n * HALF, HALF)
    mine = pl.ds(first, HALF)
    second = pl.multiple_of((1 - n) * HALF, HALF)
    theirs = pl.ds(second, HALF)
    loads = [
        pltpu.make_async_copy(src, dst, load_sem.at[i])
        for i, (src, dst) in enumerate(
            [
                (smap_hbm, smap),
                (contrib_hbm.at[0], contrib),
                (amap_hbm, amap),
                (diag_hbm.at[mine], diag),
                (mortar_hbm.at[mine], mortar),
                (inv_hbm.at[mine], inverse),
            ]
        )
    ]
    for load in loads:
        load.start()

    def exchange(src, dst, leg, c):
        for p in peers:
            pltpu.make_async_remote_copy(
                src_ref=src.at[c, p, pl.ds(0, CAP)],
                dst_ref=dst.at[c, w, pl.ds(0, CAP)],
                send_sem=send_sem.at[leg, c],
                recv_sem=recv_sem.at[leg, c],
                device_id={"wide": p},
                device_id_type=MESH,
            ).start()
        dst[c, pl.ds(w, 1)] = src[c, pl.ds(w, 1)]

    def all_bytes(buf, sem, c):
        ref = buf.at[c, pl.ds(0, N_WIDE - 1), pl.ds(0, CAP)]
        return pltpu.make_async_copy(ref, ref, sem)

    def swap(src, dst, leg, c):
        return pltpu.make_async_remote_copy(
            src_ref=src, dst_ref=dst, send_sem=xs_sem.at[leg, c], recv_sem=xr_sem.at[leg, c],
            device_id={"narrow": 1 - n}, device_id_type=MESH,
        )

    loads[0].wait()
    s_rows, s_cols = padded_map(smap)
    one_hot_cols(s_cols, s_col, ROWS)
    zero = jnp.zeros((N_WIDE, PAD - CAP, NODES), F32)
    for c in range(3):
        recv[c, :, pl.ds(CAP, PAD - CAP), :] = zero
        home[c, :, pl.ds(CAP, PAD - CAP), :] = zero
    loads[1].wait()

    for c in range(3):
        both = dot(s_col[...], split(contrib[c]))
        send[c] = (both[:, :NODES] + both[:, NODES:]).reshape(N_WIDE, PAD, NODES)
        if c == 0:
            pl.semaphore_wait(barrier, N_WIDE)
        exchange(send, recv, 0, c)

    for load in loads[2:]:
        load.wait()
    a_rows, a_cols = padded_map(amap)
    one_hot_rows(a_rows, a_row, BLK)
    one_hot_cols(a_cols, a_col, BLK)
    eye = jnp.where(
        lax.broadcasted_iota(jnp.int32, (NODES, NODES), 0)
        == lax.broadcasted_iota(jnp.int32, (NODES, NODES), 1),
        1.0,
        0.0,
    ).astype(BF16)

    @pl.loop(0, HALF // 8)
    def _(g):
        for b in range(8):
            inverse[g * 8 + b] = dot_nt(eye, inverse[g * 8 + b]).astype(BF16)
            mortar_t[g * 8 + b] = dot_nt(eye, mortar[g * 8 + b]).astype(BF16)

    one_hot_rows(s_rows, s_row, ROWS)
    sub = lax.broadcasted_iota(jnp.int32, (8, NODES), 0)

    def block_sums(c):
        all_bytes(recv, recv_sem.at[0, c], c).wait()
        both_in = split(recv[c].reshape(SLOTS, NODES))
        both = dot(a_row[theirs, :], both_in)
        sums[c, theirs, :] = both[:, :NODES] + both[:, NODES:]
        swap(sums.at[c, theirs], other.at[c], 0, c).start()
        both = dot(a_row[mine, :], both_in)
        sums[c, mine, :] = both[:, :NODES] + both[:, NODES:]

    def stage(mats, src, finish):
        @pl.loop(0, HALF // CHUNK)
        def _(g):
            for h in range(CHUNK // 8):
                at = pl.ds(pl.multiple_of(g * CHUNK + h * 8, 8), 8)
                v = src[at, :]
                total = None
                for b in range(8):
                    left = jnp.where(sub == b, v, 0.0).astype(BF16)
                    got = dot(left, mats[g * CHUNK + h * 8 + b])
                    total = got if total is None else total + got
                finish(at, total)

    def solve(c):
        swap(sums.at[c, theirs], other.at[c], 0, c).wait()
        own = sums[c, mine, :]
        got = other[c]
        vec[c] = jnp.where(n == 0, own, got) / diag[...]
        mid[c] = jnp.where(n == 0, got, own)

        def after_push(at, v):
            mid[c, at, :] = mid[c, at, :] + v

        def after_master(at, v):
            fix[c, 1, at, :] = v

        def after_slave(at, v):
            fix[c, 0, at, :] = v / diag[at, :]

        stage(mortar, vec.at[c], after_push)
        stage(inverse, mid.at[c], after_master)
        stage(mortar_t, fix.at[c, 1], after_slave)
        swap(fix.at[c, 1 - n], fixed_in.at[c], 1, c).start()

    def give_back(c):
        own = fix[c, pl.ds(n, 1)][0]
        swap(fix.at[c, 1 - n], fixed_in.at[c], 1, c).wait()
        got = fixed_in[c]
        low = jnp.where(n == 0, own, got)
        high = jnp.where(n == 0, got, own)
        full = jnp.concatenate([low, high], axis=0).astype(BF16)
        back[c] = dot(a_col[...], full).reshape(N_WIDE, PAD, NODES)
        exchange(back, home, 1, c)

    block_sums(0)
    solve(0)
    block_sums(1)
    give_back(0)
    solve(1)
    block_sums(2)
    give_back(1)
    solve(2)
    give_back(2)

    for c in range(3):
        all_bytes(home, recv_sem.at[1, c], c).wait()
        out_ref[0, c] = dot(s_row[...], home[c].reshape(SLOTS, NODES).astype(BF16))

    for c in range(3):
        all_bytes(send, send_sem.at[0, c], c).wait()
        all_bytes(back, send_sem.at[1, c], c).wait()


def shards(contributions, send_map, arrival_map, dual_diagonal, mortar, master_inverse):
    vmem = pl.BlockSpec(memory_space=pltpu.VMEM)
    hbm = pl.BlockSpec(memory_space=pltpu.HBM)
    packets = pltpu.VMEM((3, N_WIDE, PAD, NODES), F32)
    return pl.pallas_call(
        kernel,
        out_shape=jax.ShapeDtypeStruct(contributions.shape, F32),
        in_specs=[hbm] * 6,
        out_specs=vmem,
        scratch_shapes=[
            pltpu.VMEM((3, ROWS, NODES), F32),
            pltpu.VMEM((1, N_WIDE * CAP), jnp.int32),
            pltpu.VMEM((1, N_WIDE * CAP), jnp.int32),
            pltpu.VMEM((HALF, NODES), F32),
            packets, packets, packets, packets,
            pltpu.VMEM((SLOTS, ROWS), BF16),
            pltpu.VMEM((ROWS, SLOTS), BF16),
            pltpu.VMEM((SLOTS, BLK), BF16),
            pltpu.VMEM((BLK, SLOTS), BF16),
            pltpu.VMEM((HALF, NODES, NODES), BF16),
            pltpu.VMEM((HALF, NODES, NODES), BF16),
            pltpu.VMEM((HALF, NODES, NODES), BF16),
            pltpu.VMEM((3, BLK, NODES), F32),
            pltpu.VMEM((3, HALF, NODES), F32),
            pltpu.VMEM((3, HALF, NODES), F32),
            pltpu.VMEM((3, HALF, NODES), F32),
            pltpu.VMEM((3, 2, HALF, NODES), F32),
            pltpu.VMEM((3, HALF, NODES), F32),
            pltpu.SemaphoreType.DMA((6,)),
            pltpu.SemaphoreType.DMA((2, 3)),
            pltpu.SemaphoreType.DMA((2, 3)),
            pltpu.SemaphoreType.DMA((2, 3)),
            pltpu.SemaphoreType.DMA((2, 3)),
        ],
        compiler_params=pltpu.CompilerParams(
            collective_id=0, has_side_effects=True, vmem_limit_bytes=40 * 1024 * 1024
        ),
        name="mortar",
    )(*(pltpu.with_memory_space_constraint(v, pltpu.HBM) for v in (contributions, send_map, arrival_map, dual_diagonal, mortar, master_inverse)))


def solution(mesh):
    placed = (
        P("narrow", None, "wide", None),
        P("wide", None),
        P("wide", None),
        P("wide", None),
        P("wide", None, None),
        P("wide", None, None),
    )
    return jax.shard_map(
        shards,
        mesh=mesh,
        in_specs=placed,
        out_specs=P("narrow", None, "wide", None),
        check_vma=False,
    )
```

```python
import functools
import jax
import jax.numpy as jnp
from jax import lax
from jax.experimental import pallas as pl
from jax.experimental.pallas import tpu as pltpu
from jax.sharding import PartitionSpec as P

MESH = pl.DeviceIdType.MESH
F32 = jnp.float32
BF16 = jnp.bfloat16
N_WIDE = 64
CAP = 14
PAD = 16
ROWS = 512
BLK = 256
HALF = 128
NODES = 128
SLOTS = N_WIDE * PAD
CHUNK = 128
TURN = 16


def hops(o):
    return sum(min(v, 4 - v) for v in o)


OFFSETS = sorted(
    ((i // 16, (i // 4) % 4, i % 4) for i in range(1, N_WIDE)),
    key=lambda o: (-hops(o), (o[0] * 5 + o[1] * 3 + o[2] * 7) % 11),
)


def dot(a, b):
    return lax.dot_general(a, b, (((1,), (0,)), ((), ())), preferred_element_type=F32)


def dot_nt(a, b):
    return lax.dot_general(a, b, (((1,), (1,)), ((), ())), preferred_element_type=F32)


def split(x):
    hi = x.astype(BF16)
    lo = (x - hi.astype(F32)).astype(BF16)
    return jnp.concatenate([hi, lo], axis=1)


def padded_map(ref):
    x = jnp.concatenate([ref[:, 112 * r : 112 * (r + 1)] for r in range(8)], axis=0) + 1
    hi = (x >> 4).astype(F32).astype(BF16)
    lo = (x & 15).astype(F32).astype(BF16)
    i = lax.broadcasted_iota(jnp.int32, (112, 128), 0)
    l = lax.broadcasted_iota(jnp.int32, (112, 128), 1)
    q = jnp.where((i == (l >> 4) * CAP + (l & 15)) & ((l & 15) < CAP), 1.0, 0.0).astype(BF16)
    rows = dot(hi, q) * 16.0 + dot(lo, q) - 1.0
    cols = jnp.transpose(jnp.concatenate([rows] * 16, axis=0))
    return rows.astype(jnp.int32), cols.astype(jnp.int32)


def one_hot_cols(cols, out_ref, width):
    lane = lax.broadcasted_iota(jnp.int32, (128, width), 1)
    for r in range(8):
        out_ref[pl.ds(128 * r, 128), :] = jnp.where(cols[:, r : r + 1] == lane, 1.0, 0.0).astype(BF16)


def one_hot_rows(rows, out_ref, height):
    sub = lax.broadcasted_iota(jnp.int32, (height, 128), 0)
    for r in range(8):
        out_ref[:, pl.ds(128 * r, 128)] = jnp.where(rows[r : r + 1, :] == sub, 1.0, 0.0).astype(BF16)


def kernel(
    contrib_hbm, smap_hbm, amap_hbm, diag_hbm, mortar_hbm, inv_hbm, out_ref,
    contrib, smap, amap, diag, send, recv, back, home,
    s_col, s_row, a_col, a_row, mortar, mortar_t, inverse,
    sums, other, vec, mid, fix, fixed_in,
    load_sem, send_sem, recv_sem, xs_sem, xr_sem,
):
    w = lax.axis_index("wide")
    n = lax.axis_index("narrow")
    x0, z0, y0 = w // 16, (w // 4) % 4, w % 4
    xs = [(x0 + i) % 4 * 16 for i in range(4)]
    zs = [(z0 + i) % 4 * 4 for i in range(4)]
    ys = [(y0 + i) % 4 for i in range(4)]
    peers = [xs[i] + zs[j] + ys[k] for i, j, k in OFFSETS]

    first = pl.multiple_of(n * HALF, HALF)
    mine = pl.ds(first, HALF)
    second = pl.multiple_of((1 - n) * HALF, HALF)
    theirs = pl.ds(second, HALF)
    loads = [
        pltpu.make_async_copy(src, dst, load_sem.at[i])
        for i, (src, dst) in enumerate(
            [
                (smap_hbm, smap),
                (contrib_hbm.at[0], contrib),
                (amap_hbm, amap),
                (diag_hbm.at[mine], diag),
                (mortar_hbm.at[mine], mortar),
                (inv_hbm.at[mine], inverse),
            ]
        )
    ]
    for load in loads:
        load.start()

    barrier = pltpu.get_barrier_semaphore()
    for p in peers:
        pl.semaphore_signal(barrier, inc=1, device_id={"wide": p}, device_id_type=MESH)
    pl.semaphore_signal(barrier, inc=1, device_id={"narrow": 1 - n}, device_id_type=MESH)

    def exchange(src, dst, leg, c):
        for p in peers:
            pltpu.make_async_remote_copy(
                src_ref=src.at[c, p, pl.ds(0, CAP)],
                dst_ref=dst.at[c, w, pl.ds(0, CAP)],
                send_sem=send_sem.at[leg, c],
                recv_sem=recv_sem.at[leg, c],
                device_id={"wide": p},
                device_id_type=MESH,
            ).start()
        dst[c, pl.ds(w, 1)] = src[c, pl.ds(w, 1)]

    def all_bytes(buf, sem, c):
        ref = buf.at[c, pl.ds(0, N_WIDE - 1), pl.ds(0, CAP)]
        return pltpu.make_async_copy(ref, ref, sem)

    def swap(src, dst, leg, c):
        return pltpu.make_async_remote_copy(
            src_ref=src, dst_ref=dst, send_sem=xs_sem.at[leg, c], recv_sem=xr_sem.at[leg, c],
            device_id={"narrow": 1 - n}, device_id_type=MESH,
        )

    loads[0].wait()
    s_rows, s_cols = padded_map(smap)
    one_hot_cols(s_cols, s_col, ROWS)
    zero = jnp.zeros((N_WIDE, PAD - CAP, NODES), F32)
    for c in range(3):
        recv[c, :, pl.ds(CAP, PAD - CAP), :] = zero
        home[c, :, pl.ds(CAP, PAD - CAP), :] = zero
    loads[1].wait()

    def gather(c):
        both = dot(s_col[...], split(contrib[c]))
        send[c] = (both[:, :NODES] + both[:, NODES:]).reshape(N_WIDE, PAD, NODES)

    def turn(src, dst, lo, hi):
        @pl.loop(lo // TURN, hi // TURN)
        def _(g):
            for b in range(TURN):
                dst[g * TURN + b] = jnp.transpose(src[g * TURN + b])

    gather(0)
    pl.semaphore_wait(barrier, N_WIDE)
    exchange(send, recv, 0, 0)
    gather(1)
    loads[5].wait()
    turn(inverse, inverse, 0, HALF)
    loads[4].wait()
    turn(mortar, mortar_t, 0, HALF)
    all_bytes(send, send_sem.at[0, 0], 0).wait()
    exchange(send, recv, 0, 1)
    gather(2)
    loads[2].wait()
    loads[3].wait()
    a_rows, a_cols = padded_map(amap)
    one_hot_rows(a_rows, a_row, BLK)
    sub = lax.broadcasted_iota(jnp.int32, (8, NODES), 0)

    def block_sums(c):
        all_bytes(recv, recv_sem.at[0, c], c).wait()
        both_in = split(recv[c].reshape(SLOTS, NODES))
        both = dot(a_row[...], both_in)
        sums[c] = both[:, :NODES] + both[:, NODES:]
        swap(sums.at[c, theirs], other.at[c], 0, c).start()

    def stage(mats, src, finish):
        @pl.loop(0, HALF // CHUNK)
        def _(g):
            for h in range(CHUNK // 8):
                at = pl.ds(pl.multiple_of(g * CHUNK + h * 8, 8), 8)
                v = src[at, :]
                total = None
                for b in range(8):
                    left = jnp.where(sub == b, v, 0.0).astype(BF16)
                    got = dot(left, mats[g * CHUNK + h * 8 + b])
                    total = got if total is None else total + got
                finish(at, total)

    def solve(c):
        swap(sums.at[c, theirs], other.at[c], 0, c).wait()
        own = sums[c, mine, :]
        got = other[c]
        vec[c] = jnp.where(n == 0, own, got) / diag[...]
        mid[c] = jnp.where(n == 0, got, own)

        def after_push(at, v):
            mid[c, at, :] = mid[c, at, :] + v

        def after_master(at, v):
            fix[c, 1, at, :] = v

        def after_slave(at, v):
            fix[c, 0, at, :] = v / diag[at, :]

        stage(mortar, vec.at[c], after_push)
        stage(inverse, mid.at[c], after_master)
        stage(mortar_t, fix.at[c, 1], after_slave)
        swap(fix.at[c, 1 - n], fixed_in.at[c], 1, c).start()

    def give_back(c):
        own = fix[c, pl.ds(n, 1)][0]
        swap(fix.at[c, 1 - n], fixed_in.at[c], 1, c).wait()
        got = fixed_in[c]
        low = jnp.where(n == 0, own, got)
        high = jnp.where(n == 0, got, own)
        full = jnp.concatenate([low, high], axis=0).astype(BF16)
        back[c] = dot(a_col[...], full).reshape(N_WIDE, PAD, NODES)
        exchange(back, home, 1, c)

    def place(c):
        all_bytes(home, recv_sem.at[1, c], c).wait()
        out_ref[0, c] = dot(s_row[...], home[c].reshape(SLOTS, NODES).astype(BF16))

    block_sums(0)
    exchange(send, recv, 0, 2)
    one_hot_cols(a_cols, a_col, BLK)
    solve(0)
    block_sums(1)
    one_hot_rows(s_rows, s_row, ROWS)
    give_back(0)
    solve(1)
    block_sums(2)
    give_back(1)
    solve(2)
    place(0)
    give_back(2)
    place(1)
    place(2)

    for c in range(3):
        if c:
            all_bytes(send, send_sem.at[0, c], c).wait()
        all_bytes(back, send_sem.at[1, c], c).wait()


def shards(contributions, send_map, arrival_map, dual_diagonal, mortar, master_inverse):
    vmem = pl.BlockSpec(memory_space=pltpu.VMEM)
    hbm = pl.BlockSpec(memory_space=pltpu.HBM)
    packets = pltpu.VMEM((3, N_WIDE, PAD, NODES), F32)
    return pl.pallas_call(
        kernel,
        out_shape=jax.ShapeDtypeStruct(contributions.shape, F32),
        in_specs=[hbm] * 6,
        out_specs=vmem,
        scratch_shapes=[
            pltpu.VMEM((3, ROWS, NODES), F32),
            pltpu.VMEM((1, N_WIDE * CAP), jnp.int32),
            pltpu.VMEM((1, N_WIDE * CAP), jnp.int32),
            pltpu.VMEM((HALF, NODES), F32),
            packets, packets, packets, packets,
            pltpu.VMEM((SLOTS, ROWS), BF16),
            pltpu.VMEM((ROWS, SLOTS), BF16),
            pltpu.VMEM((SLOTS, BLK), BF16),
            pltpu.VMEM((BLK, SLOTS), BF16),
            pltpu.VMEM((HALF, NODES, NODES), BF16),
            pltpu.VMEM((HALF, NODES, NODES), BF16),
            pltpu.VMEM((HALF, NODES, NODES), BF16),
            pltpu.VMEM((3, BLK, NODES), F32),
            pltpu.VMEM((3, HALF, NODES), F32),
            pltpu.VMEM((3, HALF, NODES), F32),
            pltpu.VMEM((3, HALF, NODES), F32),
            pltpu.VMEM((3, 2, HALF, NODES), F32),
            pltpu.VMEM((3, HALF, NODES), F32),
            pltpu.SemaphoreType.DMA((6,)),
            pltpu.SemaphoreType.DMA((2, 3)),
            pltpu.SemaphoreType.DMA((2, 3)),
            pltpu.SemaphoreType.DMA((2, 3)),
            pltpu.SemaphoreType.DMA((2, 3)),
        ],
        compiler_params=pltpu.CompilerParams(
            collective_id=0, has_side_effects=True, vmem_limit_bytes=40 * 1024 * 1024
        ),
        name="mortar",
    )(*(pltpu.with_memory_space_constraint(v, pltpu.HBM) for v in (contributions, send_map, arrival_map, dual_diagonal, mortar, master_inverse)))


def solution(mesh):
    placed = (
        P("narrow", None, "wide", None),
        P("wide", None),
        P("wide", None),
        P("wide", None),
        P("wide", None, None),
        P("wide", None, None),
    )
    return jax.shard_map(
        shards,
        mesh=mesh,
        in_specs=placed,
        out_specs=P("narrow", None, "wide", None),
        check_vma=False,
    )
```

```python
import functools
import jax
import jax.numpy as jnp
from jax import lax
from jax.experimental import pallas as pl
from jax.experimental.pallas import tpu as pltpu
from jax.sharding import PartitionSpec as P

MESH = pl.DeviceIdType.MESH
F32 = jnp.float32
BF16 = jnp.bfloat16
N_WIDE = 64
CAP = 14
PAD = 16
ROWS = 512
BLK = 256
HALF = 128
NODES = 128
SLOTS = N_WIDE * PAD
CHUNK = 128
TURN = 16


OUT = [
    42, 26, 58, 38, 46, 43, 41, 37, 39, 59, 47, 54, 30, 62, 27, 40,
    25, 45, 22, 57, 34, 10, 44, 55, 50, 18, 23, 36, 24, 61, 9, 29,
    35, 14, 56, 6, 31, 11, 63, 33, 53, 21, 19, 49, 7, 17, 5, 52,
    28, 15, 32, 2, 20, 51, 60, 13, 8, 4, 1, 16, 12, 3, 48,
]
BACK = [
    42, 46, 41, 58, 26, 43, 38, 22, 39, 34, 45, 40, 62, 30, 57, 25,
    47, 10, 37, 59, 27, 54, 24, 14, 63, 9, 31, 36, 53, 21, 11, 6,
    33, 55, 23, 50, 18, 44, 35, 61, 29, 56, 49, 17, 7, 60, 2, 28,
    51, 19, 13, 8, 52, 15, 20, 5, 32, 4, 48, 16, 1, 12, 3,
]


def dot(a, b):
    return lax.dot_general(a, b, (((1,), (0,)), ((), ())), preferred_element_type=F32)


def dot_nt(a, b):
    return lax.dot_general(a, b, (((1,), (1,)), ((), ())), preferred_element_type=F32)


def split(x):
    hi = x.astype(BF16)
    lo = (x - hi.astype(F32)).astype(BF16)
    return jnp.concatenate([hi, lo], axis=1)


def padded_map(ref):
    x = jnp.concatenate([ref[:, 112 * r : 112 * (r + 1)] for r in range(8)], axis=0) + 1
    hi = (x >> 4).astype(F32).astype(BF16)
    lo = (x & 15).astype(F32).astype(BF16)
    i = lax.broadcasted_iota(jnp.int32, (112, 128), 0)
    l = lax.broadcasted_iota(jnp.int32, (112, 128), 1)
    q = jnp.where((i == (l >> 4) * CAP + (l & 15)) & ((l & 15) < CAP), 1.0, 0.0).astype(BF16)
    rows = dot(hi, q) * 16.0 + dot(lo, q) - 1.0
    cols = jnp.transpose(jnp.concatenate([rows] * 16, axis=0))
    return rows.astype(jnp.int32), cols.astype(jnp.int32)


def one_hot_cols(cols, out_ref, width):
    lane = lax.broadcasted_iota(jnp.int32, (128, width), 1)
    for r in range(8):
        out_ref[pl.ds(128 * r, 128), :] = jnp.where(cols[:, r : r + 1] == lane, 1.0, 0.0).astype(BF16)


def one_hot_rows(rows, out_ref, height):
    sub = lax.broadcasted_iota(jnp.int32, (height, 128), 0)
    for r in range(8):
        out_ref[:, pl.ds(128 * r, 128)] = jnp.where(rows[r : r + 1, :] == sub, 1.0, 0.0).astype(BF16)


def kernel(
    contrib_hbm, smap_hbm, amap_hbm, diag_hbm, mortar_hbm, inv_hbm, out_ref,
    contrib, smap, amap, diag, send, recv, back, home,
    s_col, s_row, a_col, a_row, mortar, mortar_t, inverse,
    sums, other, vec, mid, fix, fixed_in,
    load_sem, send_sem, recv_sem, xs_sem, xr_sem,
):
    w = lax.axis_index("wide")
    n = lax.axis_index("narrow")
    x0, z0, y0 = w // 16, (w // 4) % 4, w % 4
    xs = [(x0 + i) % 4 * 16 for i in range(4)]
    zs = [(z0 + i) % 4 * 4 for i in range(4)]
    ys = [(y0 + i) % 4 for i in range(4)]
    peers, peers_back = (
        [xs[v // 16] + zs[(v // 4) % 4] + ys[v % 4] for v in order] for order in (OUT, BACK)
    )

    first = pl.multiple_of(n * HALF, HALF)
    mine = pl.ds(first, HALF)
    second = pl.multiple_of((1 - n) * HALF, HALF)
    theirs = pl.ds(second, HALF)
    loads = [
        pltpu.make_async_copy(src, dst, load_sem.at[i])
        for i, (src, dst) in enumerate(
            [
                (smap_hbm, smap),
                (contrib_hbm.at[0], contrib),
                (amap_hbm, amap),
                (diag_hbm.at[mine], diag),
                (mortar_hbm.at[mine], mortar),
                (inv_hbm.at[mine], inverse),
            ]
        )
    ]
    for load in loads:
        load.start()

    barrier = pltpu.get_barrier_semaphore()
    for p in peers:
        pl.semaphore_signal(barrier, inc=1, device_id={"wide": p}, device_id_type=MESH)
    pl.semaphore_signal(barrier, inc=1, device_id={"narrow": 1 - n}, device_id_type=MESH)

    def exchange(src, dst, leg, c):
        for p in (peers, peers_back)[leg]:
            pltpu.make_async_remote_copy(
                src_ref=src.at[c, p, pl.ds(0, CAP)],
                dst_ref=dst.at[c, w, pl.ds(0, CAP)],
                send_sem=send_sem.at[leg, c],
                recv_sem=recv_sem.at[leg, c],
                device_id={"wide": p},
                device_id_type=MESH,
            ).start()
        dst[c, pl.ds(w, 1)] = src[c, pl.ds(w, 1)]

    def all_bytes(buf, sem, c):
        ref = buf.at[c, pl.ds(0, N_WIDE - 1), pl.ds(0, CAP)]
        return pltpu.make_async_copy(ref, ref, sem)

    def swap(src, dst, leg, c):
        return pltpu.make_async_remote_copy(
            src_ref=src, dst_ref=dst, send_sem=xs_sem.at[leg, c], recv_sem=xr_sem.at[leg, c],
            device_id={"narrow": 1 - n}, device_id_type=MESH,
        )

    loads[0].wait()
    s_rows, s_cols = padded_map(smap)
    one_hot_cols(s_cols, s_col, ROWS)
    zero = jnp.zeros((N_WIDE, PAD - CAP, NODES), F32)
    for c in range(3):
        recv[c, :, pl.ds(CAP, PAD - CAP), :] = zero
        home[c, :, pl.ds(CAP, PAD - CAP), :] = zero
    loads[1].wait()

    def gather(c):
        both = dot(s_col[...], split(contrib[c]))
        send[c] = (both[:, :NODES] + both[:, NODES:]).reshape(N_WIDE, PAD, NODES)

    def turn(src, dst, lo, hi):
        @pl.loop(lo // TURN, hi // TURN)
        def _(g):
            for b in range(TURN):
                dst[g * TURN + b] = jnp.transpose(src[g * TURN + b])

    gather(0)
    pl.semaphore_wait(barrier, N_WIDE)
    exchange(send, recv, 0, 0)
    gather(1)
    loads[5].wait()
    turn(inverse, inverse, 0, HALF)
    loads[4].wait()
    turn(mortar, mortar_t, 0, HALF)
    exchange(send, recv, 0, 1)
    gather(2)
    loads[2].wait()
    loads[3].wait()
    a_rows, a_cols = padded_map(amap)
    one_hot_rows(a_rows, a_row, BLK)
    sub = lax.broadcasted_iota(jnp.int32, (8, NODES), 0)

    def block_sums(c):
        all_bytes(recv, recv_sem.at[0, c], c).wait()
        both_in = split(recv[c].reshape(SLOTS, NODES))
        both = dot(a_row[...], both_in)
        sums[c] = both[:, :NODES] + both[:, NODES:]
        swap(sums.at[c, theirs], other.at[c], 0, c).start()

    def stage(mats, src, finish):
        @pl.loop(0, HALF // CHUNK)
        def _(g):
            for h in range(CHUNK // 8):
                at = pl.ds(pl.multiple_of(g * CHUNK + h * 8, 8), 8)
                v = src[at, :]
                total = None
                for b in range(8):
                    left = jnp.where(sub == b, v, 0.0).astype(BF16)
                    got = dot(left, mats[g * CHUNK + h * 8 + b])
                    total = got if total is None else total + got
                finish(at, total)

    def solve(c):
        swap(sums.at[c, theirs], other.at[c], 0, c).wait()
        own = sums[c, mine, :]
        got = other[c]
        vec[c] = jnp.where(n == 0, own, got) / diag[...]
        mid[c] = jnp.where(n == 0, got, own)

        def after_push(at, v):
            mid[c, at, :] = mid[c, at, :] + v

        def after_master(at, v):
            fix[c, 1, at, :] = v

        def after_slave(at, v):
            fix[c, 0, at, :] = v / diag[at, :]

        stage(mortar, vec.at[c], after_push)
        stage(inverse, mid.at[c], after_master)
        stage(mortar_t, fix.at[c, 1], after_slave)
        swap(fix.at[c, 1 - n], fixed_in.at[c], 1, c).start()

    def give_back(c):
        own = fix[c, pl.ds(n, 1)][0]
        swap(fix.at[c, 1 - n], fixed_in.at[c], 1, c).wait()
        got = fixed_in[c]
        low = jnp.where(n == 0, own, got)
        high = jnp.where(n == 0, got, own)
        full = jnp.concatenate([low, high], axis=0).astype(BF16)
        back[c] = dot(a_col[...], full).reshape(N_WIDE, PAD, NODES)
        exchange(back, home, 1, c)

    def place(c):
        all_bytes(home, recv_sem.at[1, c], c).wait()
        out_ref[0, c] = dot(s_row[...], home[c].reshape(SLOTS, NODES).astype(BF16))

    block_sums(0)
    exchange(send, recv, 0, 2)
    one_hot_cols(a_cols, a_col, BLK)
    solve(0)
    one_hot_rows(s_rows, s_row, ROWS)
    block_sums(1)
    give_back(0)
    solve(1)
    block_sums(2)
    give_back(1)
    solve(2)
    place(0)
    give_back(2)
    place(1)
    place(2)

    for c in range(3):
        all_bytes(send, send_sem.at[0, c], c).wait()
        all_bytes(back, send_sem.at[1, c], c).wait()


def shards(contributions, send_map, arrival_map, dual_diagonal, mortar, master_inverse):
    vmem = pl.BlockSpec(memory_space=pltpu.VMEM)
    hbm = pl.BlockSpec(memory_space=pltpu.HBM)
    packets = pltpu.VMEM((3, N_WIDE, PAD, NODES), F32)
    return pl.pallas_call(
        kernel,
        out_shape=jax.ShapeDtypeStruct(contributions.shape, F32),
        in_specs=[hbm] * 6,
        out_specs=vmem,
        scratch_shapes=[
            pltpu.VMEM((3, ROWS, NODES), F32),
            pltpu.VMEM((1, N_WIDE * CAP), jnp.int32),
            pltpu.VMEM((1, N_WIDE * CAP), jnp.int32),
            pltpu.VMEM((HALF, NODES), F32),
            packets, packets, packets, packets,
            pltpu.VMEM((SLOTS, ROWS), BF16),
            pltpu.VMEM((ROWS, SLOTS), BF16),
            pltpu.VMEM((SLOTS, BLK), BF16),
            pltpu.VMEM((BLK, SLOTS), BF16),
            pltpu.VMEM((HALF, NODES, NODES), BF16),
            pltpu.VMEM((HALF, NODES, NODES), BF16),
            pltpu.VMEM((HALF, NODES, NODES), BF16),
            pltpu.VMEM((3, BLK, NODES), F32),
            pltpu.VMEM((3, HALF, NODES), F32),
            pltpu.VMEM((3, HALF, NODES), F32),
            pltpu.VMEM((3, HALF, NODES), F32),
            pltpu.VMEM((3, 2, HALF, NODES), F32),
            pltpu.VMEM((3, HALF, NODES), F32),
            pltpu.SemaphoreType.DMA((6,)),
            pltpu.SemaphoreType.DMA((2, 3)),
            pltpu.SemaphoreType.DMA((2, 3)),
            pltpu.SemaphoreType.DMA((2, 3)),
            pltpu.SemaphoreType.DMA((2, 3)),
        ],
        compiler_params=pltpu.CompilerParams(
            collective_id=0, has_side_effects=True, vmem_limit_bytes=40 * 1024 * 1024
        ),
        name="mortar",
    )(*(pltpu.with_memory_space_constraint(v, pltpu.HBM) for v in (contributions, send_map, arrival_map, dual_diagonal, mortar, master_inverse)))


def solution(mesh):
    placed = (
        P("narrow", None, "wide", None),
        P("wide", None),
        P("wide", None),
        P("wide", None),
        P("wide", None, None),
        P("wide", None, None),
    )
    return jax.shard_map(
        shards,
        mesh=mesh,
        in_specs=placed,
        out_specs=P("narrow", None, "wide", None),
        check_vma=False,
    )
```

```python
import functools
import jax
import jax.numpy as jnp
from jax import lax
from jax.experimental import pallas as pl
from jax.experimental.pallas import tpu as pltpu
from jax.sharding import PartitionSpec as P

MESH = pl.DeviceIdType.MESH
F32 = jnp.float32
BF16 = jnp.bfloat16
N_WIDE = 64
CAP = 14
PAD = 16
ROWS = 512
BLK = 256
HALF = 128
NODES = 128
SLOTS = N_WIDE * PAD
CHUNK = 128
TURN = 16


OUT = [
    42, 26, 58, 38, 46, 43, 41, 37, 39, 59, 47, 54, 30, 62, 27, 40,
    25, 45, 22, 57, 34, 10, 44, 55, 50, 18, 23, 36, 24, 61, 9, 29,
    35, 14, 56, 6, 31, 11, 63, 33, 53, 21, 19, 49, 7, 17, 5, 52,
    28, 15, 32, 2, 20, 51, 60, 13, 8, 4, 1, 16, 12, 3, 48,
]
BACK = [
    42, 46, 41, 58, 26, 43, 38, 22, 39, 34, 45, 40, 62, 30, 57, 25,
    47, 10, 37, 59, 27, 54, 24, 14, 63, 9, 31, 36, 53, 21, 11, 6,
    33, 55, 23, 50, 18, 44, 35, 61, 29, 56, 49, 17, 7, 60, 2, 28,
    51, 19, 13, 8, 52, 15, 20, 5, 32, 4, 48, 16, 1, 12, 3,
]


def dot(a, b):
    return lax.dot_general(a, b, (((1,), (0,)), ((), ())), preferred_element_type=F32)


def dot_nt(a, b):
    return lax.dot_general(a, b, (((1,), (1,)), ((), ())), preferred_element_type=F32)


def split(x):
    hi = x.astype(BF16)
    lo = (x - hi.astype(F32)).astype(BF16)
    return jnp.concatenate([hi, lo], axis=1)


def padded_map(ref):
    x = jnp.concatenate([ref[:, 112 * r : 112 * (r + 1)] for r in range(8)], axis=0) + 1
    hi = (x >> 4).astype(F32).astype(BF16)
    lo = (x & 15).astype(F32).astype(BF16)
    i = lax.broadcasted_iota(jnp.int32, (112, 128), 0)
    l = lax.broadcasted_iota(jnp.int32, (112, 128), 1)
    q = jnp.where((i == (l >> 4) * CAP + (l & 15)) & ((l & 15) < CAP), 1.0, 0.0).astype(BF16)
    rows = dot(hi, q) * 16.0 + dot(lo, q) - 1.0
    cols = jnp.transpose(jnp.concatenate([rows] * 16, axis=0))
    return rows.astype(jnp.int32), cols.astype(jnp.int32)


def one_hot_cols(cols, out_ref, width):
    lane = lax.broadcasted_iota(jnp.int32, (128, width), 1)
    for r in range(8):
        out_ref[pl.ds(128 * r, 128), :] = jnp.where(cols[:, r : r + 1] == lane, 1.0, 0.0).astype(BF16)


def one_hot_rows(rows, out_ref, height):
    sub = lax.broadcasted_iota(jnp.int32, (height, 128), 0)
    for r in range(8):
        out_ref[:, pl.ds(128 * r, 128)] = jnp.where(rows[r : r + 1, :] == sub, 1.0, 0.0).astype(BF16)


def kernel(
    contrib_hbm, smap_hbm, amap_hbm, diag_hbm, mortar_hbm, inv_hbm, out_ref,
    contrib, smap, amap, diag, send, recv, back, home,
    s_col, s_row, a_col, a_row, mortar, mortar_t, inverse,
    sums, other, vec, mid, fix, fixed_in,
    load_sem, send_sem, recv_sem, xs_sem, xr_sem,
):
    w = lax.axis_index("wide")
    n = lax.axis_index("narrow")
    x0, z0, y0 = w // 16, (w // 4) % 4, w % 4
    xs = [(x0 + i) % 4 * 16 for i in range(4)]
    zs = [(z0 + i) % 4 * 4 for i in range(4)]
    ys = [(y0 + i) % 4 for i in range(4)]
    peers, peers_back = (
        [xs[v // 16] + zs[(v // 4) % 4] + ys[v % 4] for v in order] for order in (OUT, BACK)
    )

    first = pl.multiple_of(n * HALF, HALF)
    mine = pl.ds(first, HALF)
    second = pl.multiple_of((1 - n) * HALF, HALF)
    theirs = pl.ds(second, HALF)
    loads = [
        pltpu.make_async_copy(src, dst, load_sem.at[i])
        for i, (src, dst) in enumerate(
            [
                (smap_hbm, smap),
                (contrib_hbm.at[0], contrib),
                (amap_hbm, amap),
                (diag_hbm.at[mine], diag),
                (mortar_hbm.at[mine], mortar),
                (inv_hbm.at[mine], inverse),
            ]
        )
    ]
    for load in loads:
        load.start()

    barrier = pltpu.get_barrier_semaphore()
    for p in peers:
        pl.semaphore_signal(barrier, inc=1, device_id={"wide": p}, device_id_type=MESH)
    pl.semaphore_signal(barrier, inc=1, device_id={"narrow": 1 - n}, device_id_type=MESH)

    def exchange(src, dst, leg, c):
        for p in (peers, peers_back)[leg]:
            pltpu.make_async_remote_copy(
                src_ref=src.at[c, p, pl.ds(0, CAP)],
                dst_ref=dst.at[c, w, pl.ds(0, CAP)],
                send_sem=send_sem.at[leg, c],
                recv_sem=recv_sem.at[leg, c],
                device_id={"wide": p},
                device_id_type=MESH,
            ).start()
        dst[c, pl.ds(w, 1)] = src[c, pl.ds(w, 1)]

    def all_bytes(buf, sem, c):
        ref = buf.at[c, pl.ds(0, N_WIDE - 1), pl.ds(0, CAP)]
        return pltpu.make_async_copy(ref, ref, sem)

    def swap(src, dst, leg, c):
        return pltpu.make_async_remote_copy(
            src_ref=src, dst_ref=dst, send_sem=xs_sem.at[leg, c], recv_sem=xr_sem.at[leg, c],
            device_id={"narrow": 1 - n}, device_id_type=MESH,
        )

    loads[0].wait()
    s_rows, s_cols = padded_map(smap)
    one_hot_cols(s_cols, s_col, ROWS)
    zero = jnp.zeros((N_WIDE, PAD - CAP, NODES), F32)
    for c in range(3):
        recv[c, :, pl.ds(CAP, PAD - CAP), :] = zero
        home[c, :, pl.ds(CAP, PAD - CAP), :] = zero
    loads[1].wait()

    def gather(c):
        both = dot(s_col[...], split(contrib[c]))
        send[c] = (both[:, :NODES] + both[:, NODES:]).reshape(N_WIDE, PAD, NODES)

    def turn(src, dst, lo, hi):
        @pl.loop(lo // TURN, hi // TURN)
        def _(g):
            for b in range(TURN):
                dst[g * TURN + b] = jnp.transpose(src[g * TURN + b])

    gather(0)
    pl.semaphore_wait(barrier, N_WIDE)
    exchange(send, recv, 0, 0)
    gather(1)
    loads[5].wait()
    turn(inverse, inverse, 0, HALF)
    loads[4].wait()
    turn(mortar, mortar_t, 0, HALF)
    gather(2)
    exchange(send, recv, 0, 1)
    loads[2].wait()
    loads[3].wait()
    a_rows, a_cols = padded_map(amap)
    one_hot_rows(a_rows, a_row, BLK)
    sub = lax.broadcasted_iota(jnp.int32, (8, NODES), 0)

    def block_sums(c):
        all_bytes(recv, recv_sem.at[0, c], c).wait()
        both_in = split(recv[c].reshape(SLOTS, NODES))
        both = dot(a_row[...], both_in)
        sums[c] = both[:, :NODES] + both[:, NODES:]
        swap(sums.at[c, theirs], other.at[c], 0, c).start()

    def stage(mats, src, finish):
        @pl.loop(0, HALF // CHUNK)
        def _(g):
            for h in range(CHUNK // 8):
                at = pl.ds(pl.multiple_of(g * CHUNK + h * 8, 8), 8)
                v = src[at, :]
                total = None
                for b in range(8):
                    left = jnp.where(sub == b, v, 0.0).astype(BF16)
                    got = dot(left, mats[g * CHUNK + h * 8 + b])
                    total = got if total is None else total + got
                finish(at, total)

    def solve(c):
        swap(sums.at[c, theirs], other.at[c], 0, c).wait()
        own = sums[c, mine, :]
        got = other[c]
        vec[c] = jnp.where(n == 0, own, got) / diag[...]
        mid[c] = jnp.where(n == 0, got, own)

        def after_push(at, v):
            mid[c, at, :] = mid[c, at, :] + v

        def after_master(at, v):
            fix[c, 1, at, :] = v

        def after_slave(at, v):
            fix[c, 0, at, :] = v / diag[at, :]

        stage(mortar, vec.at[c], after_push)
        stage(inverse, mid.at[c], after_master)
        stage(mortar_t, fix.at[c, 1], after_slave)
        swap(fix.at[c, 1 - n], fixed_in.at[c], 1, c).start()

    def give_back(c):
        own = fix[c, pl.ds(n, 1)][0]
        swap(fix.at[c, 1 - n], fixed_in.at[c], 1, c).wait()
        got = fixed_in[c]
        low = jnp.where(n == 0, own, got)
        high = jnp.where(n == 0, got, own)
        full = jnp.concatenate([low, high], axis=0).astype(BF16)
        back[c] = dot(a_col[...], full).reshape(N_WIDE, PAD, NODES)
        exchange(back, home, 1, c)

    def place(c):
        all_bytes(home, recv_sem.at[1, c], c).wait()
        out_ref[0, c] = dot(s_row[...], home[c].reshape(SLOTS, NODES).astype(BF16)).astype(BF16)

    block_sums(0)
    exchange(send, recv, 0, 2)
    one_hot_cols(a_cols, a_col, BLK)
    solve(0)
    one_hot_rows(s_rows, s_row, ROWS)
    block_sums(1)
    give_back(0)
    solve(1)
    block_sums(2)
    give_back(1)
    solve(2)
    place(0)
    give_back(2)
    place(1)
    place(2)

    for c in range(3):
        all_bytes(send, send_sem.at[0, c], c).wait()
        all_bytes(back, send_sem.at[1, c], c).wait()


def shards(contributions, send_map, arrival_map, dual_diagonal, mortar, master_inverse):
    vmem = pl.BlockSpec(memory_space=pltpu.VMEM)
    hbm = pl.BlockSpec(memory_space=pltpu.HBM)
    packets = pltpu.VMEM((3, N_WIDE, PAD, NODES), F32)
    return pl.pallas_call(
        kernel,
        out_shape=jax.ShapeDtypeStruct(contributions.shape, BF16),
        in_specs=[hbm] * 6,
        out_specs=vmem,
        scratch_shapes=[
            pltpu.VMEM((3, ROWS, NODES), F32),
            pltpu.VMEM((1, N_WIDE * CAP), jnp.int32),
            pltpu.VMEM((1, N_WIDE * CAP), jnp.int32),
            pltpu.VMEM((HALF, NODES), F32),
            packets, packets, packets, packets,
            pltpu.VMEM((SLOTS, ROWS), BF16),
            pltpu.VMEM((ROWS, SLOTS), BF16),
            pltpu.VMEM((SLOTS, BLK), BF16),
            pltpu.VMEM((BLK, SLOTS), BF16),
            pltpu.VMEM((HALF, NODES, NODES), BF16),
            pltpu.VMEM((HALF, NODES, NODES), BF16),
            pltpu.VMEM((HALF, NODES, NODES), BF16),
            pltpu.VMEM((3, BLK, NODES), F32),
            pltpu.VMEM((3, HALF, NODES), F32),
            pltpu.VMEM((3, HALF, NODES), F32),
            pltpu.VMEM((3, HALF, NODES), F32),
            pltpu.VMEM((3, 2, HALF, NODES), F32),
            pltpu.VMEM((3, HALF, NODES), F32),
            pltpu.SemaphoreType.DMA((6,)),
            pltpu.SemaphoreType.DMA((2, 3)),
            pltpu.SemaphoreType.DMA((2, 3)),
            pltpu.SemaphoreType.DMA((2, 3)),
            pltpu.SemaphoreType.DMA((2, 3)),
        ],
        compiler_params=pltpu.CompilerParams(
            collective_id=0, has_side_effects=True, vmem_limit_bytes=40 * 1024 * 1024
        ),
        name="mortar",
    )(*(pltpu.with_memory_space_constraint(v, pltpu.HBM) for v in (contributions, send_map, arrival_map, dual_diagonal, mortar, master_inverse))).astype(F32)


def solution(mesh):
    placed = (
        P("narrow", None, "wide", None),
        P("wide", None),
        P("wide", None),
        P("wide", None),
        P("wide", None, None),
        P("wide", None, None),
    )
    return jax.shard_map(
        shards,
        mesh=mesh,
        in_specs=placed,
        out_specs=P("narrow", None, "wide", None),
        check_vma=False,
    )
```
